32 devices in a mesh: src: 8 (over z, core), cand: 4 (over y, x).
Axes of the slice: x: 2, y: 2, z: 4, core: 2. Of those that a mesh axis runs over, the one named last changes fastest.
Arguments:
- layer_input: bfloat16 [32, 128, 1024], P(('src', 'cand')), parts along dimension 0, may hold values from -16 to 16
- token_ids: int32 [32, 128], P(('src', 'cand')), parts along dimension 0, may hold values from 0 to 50264
- lengths: int32 [32], P(('src', 'cand')), parts along dimension 0, may hold values from 32 to 128
- idf_table: float32 [402120], P('src'), parts along dimension 0, may hold values from 1 to 12
- query_weight: bfloat16 [1024, 1024], P('cand'), may hold values from -0.1875 to 0.1875
- key_weight: bfloat16 [1024, 1024], P('cand'), may hold values from -0.1875 to 0.1875
- value_weight: bfloat16 [1024, 1024], P('cand'), may hold values from -0.1875 to 0.1875
- output_weight: bfloat16 [1024, 1024], P('cand'), may hold values from -0.1875 to 0.1875
Outputs:
- embedded: bfloat16 [32, 128, 1024], P(('src', 'cand')), parts along dimension 0
- pair_utility: float32 [32, 4], P(('src', 'cand')), parts along dimension 0
- expected_utility: float32 [32], P(('src', 'cand')), parts along dimension 0
The draws below stay inside these ranges and needn't reach their ends.
There are 8 independent parts, one for each index of `src`. The reference program is written for one: setup_inputs(seed, part) draws one part's arguments, and reference() takes and returns one part's arrays. A program takes and returns all parts, laid end to end along the dimension named above; an argument that names none is the same for every part. Nothing has to cross between parts.
All inputs are finite; a program needn't handle non-finite values.
Results may differ from the reference program's by a relative error of at most 0.0086.
Values may be sent and summed in bfloat16 or wider, within the bound.
A program may use at most 64 MiB of HBM per device.

```python
import math
import jax
import jax.numpy as jnp
import numpy as np
from jax import lax

D = 1024
HEADS = 16
HEAD = 64
VOCAB = 50265
L = 128
CANDS = 4


def draw_layer_input(key, part):
    base = jax.random.normal(jax.random.fold_in(key, 21), (L, D), jnp.float32)
    noise = jax.random.normal(key, (CANDS, L, D), jnp.float32)
    mixing = jax.random.uniform(jax.random.fold_in(key, 22), (CANDS, 1, 1), jnp.float32, 0.3, 0.9)
    offsets = jax.random.randint(jax.random.fold_in(key, 23), (CANDS, 1), 0, 4)
    positions = jnp.arange(L, dtype=jnp.int32)[None, :]
    source_rows = (positions + offsets) % L
    replaced = jax.random.randint(jax.random.fold_in(key, 24), (CANDS, L), 0, 10) == 0
    other_rows = jax.random.randint(jax.random.fold_in(key, 25), (CANDS, L), 0, L)
    source_rows = jnp.where(replaced, other_rows, source_rows).astype(jnp.int32)
    shared_rows = jnp.take(base, source_rows.reshape(CANDS * L), axis=0).reshape(CANDS, L, D)
    values = mixing * shared_rows + jnp.sqrt(1.0 - mixing * mixing) * noise
    values = jnp.clip(values, -4.0, 4.0)
    return values.astype(jnp.bfloat16)


def place_ends(result, key, low, top_value):
    extent = result.shape
    spot = [jax.random.randint(jax.random.fold_in(key, axis), (), 0, extent[axis]) for axis in range(len(extent))]
    result = result.at[tuple(spot)].set(low)
    longest = extent.index(max(extent))
    spot[longest] = (spot[longest] + 1) % extent[longest]
    return result.at[tuple(spot)].set(top_value)


def level_of(key, shape, shards, least, largest):
    def one(axis_at, shards_of):
        draws = jax.random.uniform(jax.random.fold_in(jax.random.fold_in(key, 6), axis_at), (shards_of,), jnp.float32, least / len(shards), largest / len(shards))
        return jnp.repeat(jnp.exp(draws), shape[axis_at] // shards_of).reshape((-1,) + (1,) * (len(shape) - axis_at - 1))

    gain = one(*shards[0])
    for cut in shards[1:]:
        gain = gain * one(*cut)
    return gain


def cumulative_ranks(amount, skew):
    portions = [(1 << 20) // math.isqrt(rank ** skew) + 1 for rank in range(1, amount + 1)]
    scale = 1 + sum(portions) // (1 << 30)
    return np.cumsum(np.array([max(1, weight // scale) for weight in portions]))


def ranked_ids(key, extent, count, skew):
    listing = cumulative_ranks(count, skew)
    lot = jax.random.randint(jax.random.fold_in(key, 1), extent, 0, int(listing[count - 1]))
    rank = jnp.searchsorted(jnp.asarray(listing, jnp.int32), lot, side="right")
    return jax.random.permutation(jax.random.fold_in(key, 2), count)[rank].astype(jnp.int32)


def gaussian(stream_key, extent, width, bound, shards=(), held_as=jnp.bfloat16):
    factor_of = level_of(stream_key, extent, shards, -0.22, 0.18) if shards else 1.0
    array = jax.random.normal(stream_key, extent, jnp.float32) * width * factor_of
    return jnp.minimum(jnp.maximum(array, -bound), bound).astype(held_as)


def setup_inputs(seed: int = 0, part: int = 0) -> dict:
    keys = jax.random.split(jax.random.key(seed), 9)
    part_keys = jax.random.split(jax.random.fold_in(keys[8], part), 9)
    return {
        "layer_input": draw_layer_input(jax.random.fold_in(jax.random.fold_in(keys[8], part), 71), part),
        "token_ids": place_ends(ranked_ids(part_keys[1], (CANDS, L), VOCAB, 2), jax.random.fold_in(part_keys[1], 3), 0, VOCAB - 1).astype(jnp.int32),
        "lengths": place_ends(jax.random.randint(part_keys[2], (CANDS,), L // 4, L + 1), jax.random.fold_in(part_keys[2], 1), L // 4, L).astype(jnp.int32),
        "idf_table": jnp.clip(jnp.exp(jax.random.uniform(part_keys[3], (VOCAB,), jnp.float32, math.log(1.0), math.log(12.0))), 1.0, 12.0),
        "query_weight": gaussian(keys[4], (D, D), D ** -0.5, 0.1875, ((0, 4),)),
        "key_weight": gaussian(keys[5], (D, D), D ** -0.5, 0.1875, ((0, 4),)),
        "value_weight": gaussian(keys[6], (D, D), D ** -0.5, 0.1875, ((0, 4),)),
        "output_weight": gaussian(keys[7], (D, D), D ** -0.5, 0.1875, ((0, 4),)),
    }


def encode(layer_input, lengths, query_weight, key_weight, value_weight, output_weight):
    flat = layer_input.reshape(CANDS * L, D)

    def project(weight):
        return jnp.dot(flat, weight, preferred_element_type=jnp.float32).astype(jnp.bfloat16)
    queries = project(query_weight).reshape(CANDS, L, HEADS, HEAD)
    key_rows = project(key_weight).reshape(CANDS, L, HEADS, HEAD)
    value_rows = project(value_weight).reshape(CANDS, L, HEADS, HEAD)
    positions = jnp.arange(L, dtype=jnp.int32)
    valid = positions[None, :] < lengths[:, None]
    scale = 1.0 / math.sqrt(HEAD)
    scores = jnp.einsum('clhe,cmhe->chlm', queries.astype(jnp.float32), key_rows.astype(jnp.float32), precision=lax.Precision.HIGHEST) * scale
    scores = jnp.where(valid[:, None, None, :], scores, -1000000000.0)
    highest = lax.optimization_barrier(jnp.max(scores, axis=-1, keepdims=True))
    expo = jnp.exp(scores - highest)
    probs = (expo / lax.optimization_barrier(jnp.sum(expo, axis=-1, keepdims=True))).astype(jnp.bfloat16)
    context = jnp.einsum('chlm,cmhe->clhe', probs.astype(jnp.float32), value_rows.astype(jnp.float32), precision=lax.Precision.HIGHEST).astype(jnp.bfloat16).reshape(CANDS * L, D)
    mixed = jnp.dot(context, output_weight, preferred_element_type=jnp.float32) + flat.astype(jnp.float32)
    centred = mixed - lax.optimization_barrier(jnp.mean(mixed, axis=-1, keepdims=True))
    squares = lax.optimization_barrier(jnp.sum(centred * centred, axis=-1, keepdims=True))
    embedded = (centred / jnp.sqrt(squares + 0.001)).astype(jnp.bfloat16)
    return (embedded.reshape(CANDS, L, D), valid)

def reference(layer_input, token_ids, lengths, idf_table, query_weight, key_weight, value_weight, output_weight):
    embedded, valid = encode(layer_input, lengths, query_weight, key_weight, value_weight, output_weight)
    token_weight = (jnp.take(idf_table, token_ids, axis=0) * valid.astype(jnp.float32)).astype(jnp.bfloat16)
    flat_vectors = embedded.reshape(CANDS * L, D).astype(jnp.float32)
    similarity = jnp.dot(flat_vectors, flat_vectors.T, precision=lax.Precision.HIGHEST).reshape(CANDS, L, CANDS, L)
    usable = token_weight > 0
    best_other = lax.optimization_barrier(jnp.max(jnp.where(usable[None, None, :, :], similarity, -4.0), axis=3))
    weight_float = token_weight.astype(jnp.float32)
    forward = jnp.einsum('il,ilj->ij', weight_float, best_other, precision=lax.Precision.HIGHEST)
    forward = forward / lax.optimization_barrier(jnp.sum(weight_float, axis=1))[:, None]
    pair_utility = 0.5 * (forward + forward.T)
    diagonal = jnp.diagonal(pair_utility)
    expected_utility = (lax.optimization_barrier(jnp.sum(pair_utility, axis=1)) - diagonal) / (CANDS - 1)
    return (embedded, pair_utility, expected_utility)
```

```python
import functools
import math

import jax
import jax.numpy as jnp
from jax import lax
from jax.experimental import pallas as pl
from jax.experimental.pallas import tpu as pltpu
from jax.sharding import PartitionSpec as P

HEAD = 64


def block_utility(own_vectors, own_weight, far_vectors, far_weight):
    own_count, length, width = own_vectors.shape
    far_count = far_vectors.shape[0]
    similar = lax.dot_general(
        own_vectors.reshape(own_count * length, width),
        far_vectors.reshape(far_count * length, width),
        (((1,), (1,)), ((), ())),
        preferred_element_type=jnp.float32,
    )
    similar = similar.reshape(own_count, length, far_count, length)
    own_usable = own_weight > 0
    far_usable = far_weight > 0
    best_far = jnp.max(jnp.where(far_usable[None, None, :, :], similar, -4.0), axis=3)
    best_own = jnp.max(jnp.where(own_usable[:, :, None, None], similar, -4.0), axis=1)
    own_float = own_weight.astype(jnp.float32)
    far_float = far_weight.astype(jnp.float32)
    forward = jnp.einsum("il,ilj->ij", own_float, best_far, precision=lax.Precision.HIGHEST)
    forward = forward / jnp.sum(own_float, axis=1)[:, None]
    backward = jnp.einsum("jm,ijm->ij", far_float, best_own, precision=lax.Precision.HIGHEST)
    backward = backward / jnp.sum(far_float, axis=1)[None, :]
    return 0.5 * (forward + backward)


def gathered_shards(
    layer_input,
    token_ids,
    lengths,
    idf_table,
    query_weight,
    key_weight,
    value_weight,
    output_weight,
):
    local_cands, length, width = layer_input.shape
    cycle_size = lax.axis_size("cand")
    all_cands = local_cands * cycle_size
    head_size = HEAD
    head_count = width // head_size
    flat = layer_input.reshape(local_cands * length, width)
    pieces = (
        lax.all_gather(query_weight, "cand", axis=0, tiled=True),
        lax.all_gather(key_weight, "cand", axis=0, tiled=True),
        lax.all_gather(value_weight, "cand", axis=0, tiled=True),
    )
    columns = flat
    queries, key_rows, value_rows = tuple(
        (jnp.dot(columns, piece, preferred_element_type=jnp.float32) for piece in pieces)
    )
    queries = queries.astype(jnp.bfloat16).reshape(local_cands, length, head_count, head_size)
    key_rows = key_rows.astype(jnp.bfloat16).reshape(local_cands, length, head_count, head_size)
    value_rows = value_rows.astype(jnp.bfloat16).reshape(local_cands, length, head_count, head_size)
    positions = jnp.arange(length, dtype=jnp.int32)
    valid = positions[None, :] < lengths[:, None]
    scale = 1.0 / math.sqrt(head_size)
    scores = (
        jnp.einsum("clhe,cmhe->chlm", queries, key_rows, preferred_element_type=jnp.float32) * scale
    )
    scores = jnp.where(valid[:, None, None, :], scores, -1000000000.0)
    highest = jnp.max(scores, axis=-1, keepdims=True)
    expo = jnp.exp(scores - highest)
    probs = (expo / jnp.sum(expo, axis=-1, keepdims=True)).astype(jnp.bfloat16)
    context = jnp.einsum("chlm,cmhe->clhe", probs, value_rows, preferred_element_type=jnp.float32)
    context = context.astype(jnp.bfloat16).reshape(local_cands * length, width)
    columns = context
    mixed = jnp.dot(
        columns,
        lax.all_gather(output_weight, "cand", axis=0, tiled=True),
        preferred_element_type=jnp.float32,
    ) + flat.astype(jnp.float32)
    centred = mixed - jnp.mean(mixed, axis=-1, keepdims=True)
    squares = jnp.sum(centred * centred, axis=-1, keepdims=True)
    embedded = (
        (centred / jnp.sqrt(squares + 0.001))
        .astype(jnp.bfloat16)
        .reshape(local_cands, length, width)
    )
    token_weight = (jnp.take(idf_table, token_ids, axis=0) * valid.astype(jnp.float32)).astype(
        jnp.bfloat16
    )
    myself = lax.axis_index("cand")
    piece = (
        lax.all_gather(embedded, "cand", axis=0, tiled=True),
        lax.all_gather(token_weight, "cand", axis=0, tiled=True),
    )
    utility = block_utility(embedded, token_weight, piece[0], piece[1])
    blocks = utility.reshape(local_cands, cycle_size, local_cands)
    own_part = lax.dynamic_slice(blocks, (0, myself, 0), (local_cands, 1, local_cands))[:, 0, :]
    diagonal = jnp.diagonal(own_part)
    expected_utility = (jnp.sum(utility, axis=1) - diagonal) / (all_cands - 1)
    return (embedded, utility, expected_utility)


def remote(src_ref, dst_ref, send_sem, recv_sem, device):
    return pltpu.make_async_remote_copy(
        src_ref=src_ref,
        dst_ref=dst_ref,
        send_sem=send_sem,
        recv_sem=recv_sem,
        device_id=device,
        device_id_type=pl.DeviceIdType.MESH,
    )


def flipped(index, bits):
    result = index
    place = 1
    while place <= bits:
        if bits & place:
            digit = lax.rem(lax.div(index, place), 2)
            result = result + place - 2 * place * digit
        place *= 2
    return result


def kernel(
    count,
    x_hbm,
    ids_hbm,
    used,
    table_hbm,
    q_hbm,
    k_hbm,
    v_hbm,
    o_hbm,
    embedded_ref,
    utility_ref,
    expected_ref,
    stage,
    full,
    out_full,
    x_all,
    meta,
    context,
    total,
    ids,
    table,
    local_sem,
    send_sem,
    recv_sem,
):
    group, me = lax.axis_index("src"), lax.axis_index("cand")
    share = lax.rem(group, 4)
    sibling = (flipped(group, 1), me)
    mate = (flipped(group, 2), me)
    others = range(1, count)
    peer = [(group, flipped(me, bits)) for bits in range(count)]
    length, width = x_hbm.shape
    rows, columns = stage.shape[1], full.shape[2]
    quarter = rows // 4
    started = []

    def push(src_ref, dst_ref, device):
        number = len(started)
        copy = remote(src_ref, dst_ref, send_sem.at[number], recv_sem.at[number], device)
        copy.start()
        started.append(copy)
        return copy

    def column_block(index):
        return pl.ds(pl.multiple_of(index * columns, columns), columns)

    def row_block(index):
        return pl.ds(pl.multiple_of(index * rows, rows), rows)

    def row_share(index, which):
        return pl.ds(pl.multiple_of(index * rows + which * quarter, quarter), quarter)

    own_share = pl.ds(pl.multiple_of(share * quarter, quarter), quarter)
    mate_share = lax.rem(share + 2, 4)

    weights = (q_hbm, k_hbm, v_hbm)
    loads = [pltpu.make_async_copy(w, stage.at[t], local_sem.at[t]) for t, w in enumerate(weights)]
    loads += [
        pltpu.make_async_copy(o_hbm, out_full.at[row_block(me), :], local_sem.at[3]),
        pltpu.make_async_copy(x_hbm, x_all.at[0], local_sem.at[4]),
        pltpu.make_async_copy(ids_hbm, ids, local_sem.at[5]),
    ]
    loads += [
        pltpu.make_async_copy(
            w.at[:, column_block(me)], full.at[t, row_block(me), :], local_sem.at[6 + t]
        )
        for t, w in enumerate(weights)
    ]
    loads += [
        pltpu.make_async_copy(table_hbm, table, local_sem.at[9]),
    ]
    for load in loads:
        load.start()

    barrier = pltpu.get_barrier_semaphore()
    targets = [sibling, mate] + [peer[r] for r in others]
    for target in targets:
        pl.semaphore_signal(barrier, inc=1, device_id=target, device_id_type=pl.DeviceIdType.MESH)
    pl.semaphore_wait(barrier, len(targets))

    def exchange(slot):
        first = {1: push(slot(0, 0), slot(1, 0), peer[1]), 2: push(slot(0, 1), slot(2, 1), peer[2])}
        second = {
            1: push(slot(0, 1), slot(1, 1), peer[1]),
            2: push(slot(0, 0), slot(2, 0), peer[2]),
        }

        def relay():
            first[1].wait_recv()
            near = push(slot(1, 0), slot(3, 0), peer[2])
            first[2].wait_recv()
            return (near, push(slot(2, 1), slot(3, 1), peer[1]))

        return second, relay

    for load in loads[:3]:
        load.wait()
    w_copies = {}
    for r in others:
        w_copies[r] = push(
            stage.at[:, own_share, column_block(peer[r][1])],
            full.at[:, row_share(me, share), :],
            peer[r],
        )
    for load in loads[3:6]:
        load.wait()
    half = length // 2
    x_second, x_relay = exchange(lambda r, which: x_all.at[r, pl.ds(which * half, half), :])

    def out_part(r, which, part):
        start = (flipped(me, r) * rows) + which * quarter + part * (quarter // 2)
        return out_full.at[pl.ds(pl.multiple_of(start, quarter // 2), quarter // 2), :]

    def out_push(r, part, device):
        return push(out_part(r, share, part), out_part(r, share, part), device)

    o_first = {1: out_push(0, 0, peer[1]), 2: out_push(0, 1, peer[2])}
    o_second = {1: out_push(0, 1, peer[1]), 2: out_push(0, 0, peer[2])}
    for load in loads[6:]:
        load.wait()

    position = lax.broadcasted_iota(jnp.int32, (1, length), 1)

    def look_up(at, weights_row):
        return jnp.where(position == at, table[ids[0, at]], weights_row)

    valid_row = (position < used[0]).astype(jnp.float32)
    weights_row = lax.fori_loop(0, length, look_up, jnp.zeros((1, length), jnp.float32), unroll=8)
    weights_row = (weights_row * valid_row).astype(jnp.bfloat16).astype(jnp.float32)
    meta[0] = jnp.concatenate([weights_row, jnp.broadcast_to(valid_row, (7, length))], axis=0)
    m_copies = {r: push(meta.at[0], meta.at[r], peer[r]) for r in others}

    def full_share(r, which):
        return full.at[:, row_share(peer[r][1], which), :]

    def out_share(r, which):
        return out_full.at[row_share(peer[r][1], which), :]

    def spread(landed):
        return (push(landed, landed, mate), push(landed, landed, sibling))

    def hand_over(copy, landed):
        copy.wait_recv()
        return push(landed, landed, sibling)

    w_spread = {}
    for r in others:
        w_copies[r].wait_recv()
        w_spread[r] = spread(full_share(r, share))
    x_far = x_relay()
    w_hand = {r: hand_over(w_spread[r][0], full_share(r, mate_share)) for r in others}
    for r in others:
        w_spread[r][1].wait_recv()
        w_hand[r].wait_recv()

    lane = lax.broadcasted_iota(jnp.int32, (1, 2 * HEAD), 1)
    scale = 1.0 / math.sqrt(HEAD)
    first = (lane < HEAD).astype(jnp.float32)
    keep = [(first * scale).astype(jnp.bfloat16), ((1.0 - first) * scale).astype(jnp.bfloat16)]

    def context_of(r):
        rows_in = x_all[r]
        queries, key_rows, value_rows = tuple(
            jnp.dot(rows_in, full[t], preferred_element_type=jnp.float32).astype(jnp.bfloat16)
            for t in range(3)
        )
        valid = meta[r, 1:2, :] > 0.0
        pieces = []
        for start in range(0, columns, 2 * HEAD):
            span = slice(start, start + 2 * HEAD)
            q_pair, k_pair, v_pair = queries[:, span], key_rows[:, span], value_rows[:, span]
            stacked = jnp.concatenate([q_pair * keep[0], q_pair * keep[1]], axis=0)
            scores = lax.dot_general(
                stacked, k_pair, (((1,), (1,)), ((), ())), preferred_element_type=jnp.float32
            )
            scores = jnp.where(valid, scores, -1000000000.0)
            expo = jnp.exp(scores - jnp.max(scores, axis=-1, keepdims=True))
            total = jnp.sum(expo, axis=-1, keepdims=True)
            summed = jnp.dot(
                expo.astype(jnp.bfloat16), v_pair, preferred_element_type=jnp.float32
            )
            summed = summed / total
            pieces.append(jnp.where(lane < HEAD, summed[:length], summed[length:]))
        return jnp.concatenate(pieces, axis=1).astype(jnp.bfloat16)

    def context_part(r, candidate, part):
        return context.at[r, candidate, pl.ds(part * half, half), :]

    def context_push(r, candidate, part, way):
        return push(
            context_part(r, candidate, part),
            context_part(r ^ way, candidate ^ way, part),
            peer[way],
        )

    c_first, c_second = {}, {}

    def attend(r):
        context[0, r] = context_of(r)
        c_first[r] = {1: context_push(0, r, 0, 1), 2: context_push(0, r, 1, 2)}
        c_second[r] = {1: context_push(0, r, 1, 1), 2: context_push(0, r, 0, 2)}

    attend(0)
    for r in (1, 2):
        m_copies[r].wait_recv()
        x_second[r].wait_recv()
        attend(r)
    o_first[1].wait_recv()
    o_near = out_push(1, 0, peer[2])
    o_first[2].wait_recv()
    o_far = out_push(2, 1, peer[1])
    o_spread = {}
    for r in (1, 2):
        o_second[r].wait_recv()
        o_spread[r] = spread(out_share(r, share))
    m_copies[3].wait_recv()
    for copy in x_far:
        copy.wait_recv()
    attend(3)
    for copy in (o_near, o_far):
        copy.wait_recv()
    o_spread[3] = spread(out_share(3, share))

    c_near, c_far = {}, {}
    for r in range(count):
        c_first[r][1].wait_recv()
        c_near[r ^ 1] = context_push(1, r ^ 1, 0, 2)
        c_first[r][2].wait_recv()
        c_far[r ^ 2] = context_push(2, r ^ 2, 1, 1)
    o_hand = {r: hand_over(o_spread[r][0], out_share(r, mate_share)) for r in others}

    def out_rows(r):
        return out_full[row_block(peer[r][1]), :]

    def product(r):
        return jnp.dot(
            context[r].reshape(count * length, columns),
            out_rows(r),
            preferred_element_type=jnp.float32,
        ).reshape(count, length, width)

    total[...] = product(0)
    for r in (1, 2):
        o_spread[r][1].wait_recv()
        o_hand[r].wait_recv()
        for candidate in range(count):
            c_second[candidate][r].wait_recv()
        total[...] += product(r)
    o_spread[3][1].wait_recv()
    o_hand[3].wait_recv()

    own_weight = meta[0, 0:1, :]
    own_column = jnp.broadcast_to(own_weight, (length, length)).T
    own_total = jnp.sum(own_weight, axis=1, keepdims=True)
    slot = lax.broadcasted_iota(jnp.int32, utility_ref.shape, 1)

    def vectors_of(r):
        mixed = total[r] + jnp.dot(
            context[3, r], out_rows(3), preferred_element_type=jnp.float32
        )
        mixed = mixed + x_all[r].astype(jnp.float32)
        centred = mixed - jnp.mean(mixed, axis=-1, keepdims=True)
        squares = jnp.sum(centred * centred, axis=-1, keepdims=True)
        return (centred / jnp.sqrt(squares + 0.001)).astype(jnp.bfloat16)

    def pair_of(own, far, r):
        far_weight = meta[r, 0:1, :]
        similar = lax.dot_general(
            own, far, (((1,), (1,)), ((), ())), preferred_element_type=jnp.float32
        )
        best_far = jnp.max(jnp.where(far_weight > 0, similar, -4.0), axis=1, keepdims=True)
        best_own = jnp.max(jnp.where(own_column > 0, similar, -4.0), axis=0, keepdims=True)
        forward = jnp.sum(own_column[:, 0:1] * best_far, axis=0, keepdims=True) / own_total
        backward = jnp.sum(far_weight * best_own, axis=1, keepdims=True) / jnp.sum(
            far_weight, axis=1, keepdims=True
        )
        return 0.5 * (forward + backward)

    vectors = {}
    for r in (3, 2, 1, 0):
        c_near[r ^ 2].wait_recv()
        c_far[r ^ 1].wait_recv()
        vectors[r] = vectors_of(r)
    own = vectors[0]
    embedded_ref[...] = own
    utility = jnp.zeros(utility_ref.shape, jnp.float32)
    everything = jnp.zeros(expected_ref.shape, jnp.float32)
    for r in range(count):
        pair = pair_of(own, vectors[r], r)
        utility = jnp.where(slot == peer[r][1], pair, utility)
        if r:
            everything = everything + pair
    utility_ref[...] = utility
    expected_ref[...] = everything / (count - 1)

    for copy in started:
        copy.wait_send()


def shards(
    sizes,
    layer_input,
    token_ids,
    lengths,
    idf_table,
    query_weight,
    key_weight,
    value_weight,
    output_weight,
):
    local_cands, length, width = layer_input.shape
    count = sizes["cand"]
    rows = query_weight.shape[0]
    columns = width // count
    if (
        local_cands != 1
        or count != 4
        or sizes["src"] % 4
        or columns % (2 * HEAD)
        or rows % 64
        or length != 128
    ):
        return gathered_shards(
            layer_input,
            token_ids,
            lengths,
            idf_table,
            query_weight,
            key_weight,
            value_weight,
            output_weight,
        )
    anywhere = pl.BlockSpec(memory_space=pl.ANY)
    in_vmem = pl.BlockSpec(memory_space=pltpu.VMEM)
    copies = pltpu.SemaphoreType.DMA((72,))
    embedded, utility, expected = pl.pallas_call(
        functools.partial(kernel, count),
        out_shape=(
            pltpu.VMEM((length, width), jnp.bfloat16),
            pltpu.VMEM((1, count), jnp.float32),
            pltpu.VMEM((1, 1), jnp.float32),
        ),
        in_specs=[anywhere] * 2 + [pl.BlockSpec(memory_space=pltpu.SMEM)] + [anywhere] * 5,
        out_specs=(in_vmem, in_vmem, in_vmem),
        scratch_shapes=[
            pltpu.VMEM((3, rows, width), jnp.bfloat16),
            pltpu.VMEM((3, rows * count, columns), jnp.bfloat16),
            pltpu.VMEM((rows * count, width), jnp.bfloat16),
            pltpu.VMEM((count, length, width), jnp.bfloat16),
            pltpu.VMEM((count, 8, length), jnp.float32),
            pltpu.VMEM((count, count, length, columns), jnp.bfloat16),
            pltpu.VMEM((count, length, width), jnp.float32),
            pltpu.SMEM((1, length), jnp.int32),
            pltpu.SMEM(idf_table.shape, jnp.float32),
            pltpu.SemaphoreType.DMA((10,)),
            copies,
            copies,
        ],
        compiler_params=pltpu.CompilerParams(collective_id=0, has_side_effects=True),
    )(
        layer_input.reshape(length, width),
        token_ids,
        lengths,
        idf_table,
        query_weight,
        key_weight,
        value_weight,
        output_weight,
    )
    return (embedded.reshape(1, length, width), utility, expected.reshape(1))


def solution(mesh):
    in_specs = (
        P(("src", "cand"), None, None),
        P(("src", "cand"), None),
        P(("src", "cand")),
        P("src"),
        P("cand", None),
        P("cand", None),
        P("cand", None),
        P("cand", None),
    )
    out_specs = (P(("src", "cand"), None, None), P(("src", "cand"), None), P(("src", "cand")))
    return jax.shard_map(
        functools.partial(shards, dict(mesh.shape)),
        mesh=mesh,
        in_specs=in_specs,
        out_specs=out_specs,
        check_vma=False,
    )
```

```python
import functools
import math

import jax
import jax.numpy as jnp
from jax import lax
from jax.experimental import pallas as pl
from jax.experimental.pallas import tpu as pltpu
from jax.sharding import PartitionSpec as P

HEAD = 64
SLOTS = 40


def block_utility(own_vectors, own_weight, far_vectors, far_weight):
    own_count, length, width = own_vectors.shape
    far_count = far_vectors.shape[0]
    similar = lax.dot_general(
        own_vectors.reshape(own_count * length, width),
        far_vectors.reshape(far_count * length, width),
        (((1,), (1,)), ((), ())),
        preferred_element_type=jnp.float32,
    )
    similar = similar.reshape(own_count, length, far_count, length)
    own_usable = own_weight > 0
    far_usable = far_weight > 0
    best_far = jnp.max(jnp.where(far_usable[None, None, :, :], similar, -4.0), axis=3)
    best_own = jnp.max(jnp.where(own_usable[:, :, None, None], similar, -4.0), axis=1)
    own_float = own_weight.astype(jnp.float32)
    far_float = far_weight.astype(jnp.float32)
    forward = jnp.einsum("il,ilj->ij", own_float, best_far, precision=lax.Precision.HIGHEST)
    forward = forward / jnp.sum(own_float, axis=1)[:, None]
    backward = jnp.einsum("jm,ijm->ij", far_float, best_own, precision=lax.Precision.HIGHEST)
    backward = backward / jnp.sum(far_float, axis=1)[None, :]
    return 0.5 * (forward + backward)


def gathered_shards(
    layer_input,
    token_ids,
    lengths,
    idf_table,
    query_weight,
    key_weight,
    value_weight,
    output_weight,
):
    local_cands, length, width = layer_input.shape
    cycle_size = lax.axis_size("cand")
    all_cands = local_cands * cycle_size
    head_size = HEAD
    head_count = width // head_size
    flat = layer_input.reshape(local_cands * length, width)
    pieces = (
        lax.all_gather(query_weight, "cand", axis=0, tiled=True),
        lax.all_gather(key_weight, "cand", axis=0, tiled=True),
        lax.all_gather(value_weight, "cand", axis=0, tiled=True),
    )
    columns = flat
    queries, key_rows, value_rows = tuple(
        (jnp.dot(columns, piece, preferred_element_type=jnp.float32) for piece in pieces)
    )
    queries = queries.astype(jnp.bfloat16).reshape(local_cands, length, head_count, head_size)
    key_rows = key_rows.astype(jnp.bfloat16).reshape(local_cands, length, head_count, head_size)
    value_rows = value_rows.astype(jnp.bfloat16).reshape(local_cands, length, head_count, head_size)
    positions = jnp.arange(length, dtype=jnp.int32)
    valid = positions[None, :] < lengths[:, None]
    scale = 1.0 / math.sqrt(head_size)
    scores = (
        jnp.einsum("clhe,cmhe->chlm", queries, key_rows, preferred_element_type=jnp.float32) * scale
    )
    scores = jnp.where(valid[:, None, None, :], scores, -1000000000.0)
    highest = jnp.max(scores, axis=-1, keepdims=True)
    expo = jnp.exp(scores - highest)
    probs = (expo / jnp.sum(expo, axis=-1, keepdims=True)).astype(jnp.bfloat16)
    context = jnp.einsum("chlm,cmhe->clhe", probs, value_rows, preferred_element_type=jnp.float32)
    context = context.astype(jnp.bfloat16).reshape(local_cands * length, width)
    columns = context
    mixed = jnp.dot(
        columns,
        lax.all_gather(output_weight, "cand", axis=0, tiled=True),
        preferred_element_type=jnp.float32,
    ) + flat.astype(jnp.float32)
    centred = mixed - jnp.mean(mixed, axis=-1, keepdims=True)
    squares = jnp.sum(centred * centred, axis=-1, keepdims=True)
    embedded = (
        (centred / jnp.sqrt(squares + 0.001))
        .astype(jnp.bfloat16)
        .reshape(local_cands, length, width)
    )
    token_weight = (jnp.take(idf_table, token_ids, axis=0) * valid.astype(jnp.float32)).astype(
        jnp.bfloat16
    )
    myself = lax.axis_index("cand")
    piece = (
        lax.all_gather(embedded, "cand", axis=0, tiled=True),
        lax.all_gather(token_weight, "cand", axis=0, tiled=True),
    )
    utility = block_utility(embedded, token_weight, piece[0], piece[1])
    blocks = utility.reshape(local_cands, cycle_size, local_cands)
    own_part = lax.dynamic_slice(blocks, (0, myself, 0), (local_cands, 1, local_cands))[:, 0, :]
    diagonal = jnp.diagonal(own_part)
    expected_utility = (jnp.sum(utility, axis=1) - diagonal) / (all_cands - 1)
    return (embedded, utility, expected_utility)


def remote(src_ref, dst_ref, send_sem, recv_sem, device):
    return pltpu.make_async_remote_copy(
        src_ref=src_ref,
        dst_ref=dst_ref,
        send_sem=send_sem,
        recv_sem=recv_sem,
        device_id=device,
        device_id_type=pl.DeviceIdType.MESH,
    )


def flipped(index, bits):
    result = index
    place = 1
    while place <= bits:
        if bits & place:
            digit = lax.rem(lax.div(index, place), 2)
            result = result + place - 2 * place * digit
        place *= 2
    return result


def kernel(
    count,
    x_hbm,
    ids_hbm,
    used_hbm,
    table_hbm,
    q_hbm,
    k_hbm,
    v_hbm,
    o_hbm,
    embedded_ref,
    utility_ref,
    expected_ref,
    stage,
    full,
    out_full,
    x_all,
    meta,
    context,
    total,
    drain,
    ids,
    used,
    table,
    local_sem,
    send_sem,
    recv_sem,
    ready_sem,
):
    group, me = lax.axis_index("src"), lax.axis_index("cand")
    share = lax.rem(group, 4)
    sibling = (flipped(group, 1), me)
    mate = (flipped(group, 2), me)
    others = range(1, count)
    peer = [(group, flipped(me, bits)) for bits in range(count)]
    length, width = x_hbm.shape
    rows, columns = stage.shape[1], full.shape[2]
    quarter, half = rows // 4, length // 2
    sent, slots = [], []

    def signal(semaphore, device):
        pl.semaphore_signal(
            semaphore, inc=1, device_id=device, device_id_type=pl.DeviceIdType.MESH
        )

    def slot():
        slots.append(len(slots))
        return slots[-1]

    def push(src_ref, dst_ref, device, number):
        remote(src_ref, dst_ref, send_sem.at[0], recv_sem.at[number], device).start()
        sent.append(math.prod(src_ref.shape) * src_ref.dtype.itemsize)

    def landed(number, like):
        pltpu.make_async_copy(like, like, recv_sem.at[number]).wait()

    def column_block(index):
        return pl.ds(pl.multiple_of(index * columns, columns), columns)

    def row_block(index):
        return pl.ds(pl.multiple_of(index * rows, rows), rows)

    def row_share(index, which):
        return pl.ds(pl.multiple_of(index * rows + which * quarter, quarter), quarter)

    own_share = pl.ds(pl.multiple_of(share * quarter, quarter), quarter)
    mate_share = lax.rem(share + 2, 4)

    weights = (q_hbm, k_hbm, v_hbm)
    own_rows = out_full.at[row_block(me), :]
    own_block = full.at[:, row_block(me), :]
    for t, w in enumerate(weights):
        pltpu.make_async_copy(w, stage.at[t], local_sem.at[0]).start()
    load_o = pltpu.make_async_copy(o_hbm, own_rows, local_sem.at[1])
    load_x = pltpu.make_async_copy(x_hbm, x_all.at[0], local_sem.at[2])
    small = [
        pltpu.make_async_copy(used_hbm, used, local_sem.at[3]),
        pltpu.make_async_copy(ids_hbm, ids, local_sem.at[4]),
        pltpu.make_async_copy(table_hbm, table, local_sem.at[5]),
    ]
    load_o.start()
    load_x.start()
    for load in small:
        load.start()
    for t, w in enumerate(weights):
        pltpu.make_async_copy(
            w.at[:, column_block(me)], full.at[t, row_block(me), :], local_sem.at[6]
        ).start()

    barrier = pltpu.get_barrier_semaphore()
    targets = [sibling, mate, peer[1], peer[2]]
    for target in targets:
        signal(barrier, target)
    pl.semaphore_wait(barrier, len(targets))
    signal(ready_sem, peer[1])

    def full_share(r, which):
        return full.at[:, row_share(peer[r][1], which), :]

    def out_share(r, which):
        return out_full.at[row_share(peer[r][1], which), :]

    def out_part(r, part):
        start = peer[r][1] * rows + share * quarter + part * (quarter // 2)
        return out_full.at[pl.ds(pl.multiple_of(start, quarter // 2), quarter // 2), :]

    def x_part(r, part):
        return x_all.at[r, pl.ds(part * half, half), :]

    w_slot = {r: slot() for r in others}

    def send_weights(r):
        push(
            stage.at[:, own_share, column_block(peer[r][1])],
            full_share(0, share),
            peer[r],
            w_slot[r],
        )

    pltpu.make_async_copy(stage, stage, local_sem.at[0]).wait()
    send_weights(1)
    send_weights(2)
    pl.semaphore_wait(ready_sem, 1)
    send_weights(3)
    load_o.wait()
    o_first, o_second = {1: slot(), 2: slot()}, {1: slot(), 2: slot()}
    push(out_part(0, 0), out_part(0, 0), peer[1], o_first[1])
    push(out_part(0, 1), out_part(0, 1), peer[2], o_first[2])
    push(out_part(0, 1), out_part(0, 1), peer[1], o_second[1])
    push(out_part(0, 0), out_part(0, 0), peer[2], o_second[2])
    load_x.wait()
    x_first, x_second = {1: slot(), 2: slot()}, {1: slot(), 2: slot()}
    push(x_part(0, 0), x_part(1, 0), peer[1], x_first[1])
    push(x_part(0, 1), x_part(2, 1), peer[2], x_first[2])
    push(x_part(0, 1), x_part(1, 1), peer[1], x_second[1])
    push(x_part(0, 0), x_part(2, 0), peer[2], x_second[2])

    position = lax.broadcasted_iota(jnp.int32, (1, length), 1)

    def look_up(at, weights_row):
        return jnp.where(position == at, table[ids[0, at]], weights_row)

    for load in small:
        load.wait()
    valid_row = (position < used[0]).astype(jnp.float32)
    weights_row = lax.fori_loop(0, length, look_up, jnp.zeros((1, length), jnp.float32), unroll=8)
    weights_row = (weights_row * valid_row).astype(jnp.bfloat16).astype(jnp.float32)
    meta[0] = jnp.concatenate([weights_row, jnp.broadcast_to(valid_row, (7, length))], axis=0)
    m_slot = slot()
    for r in others:
        push(meta.at[0], meta.at[r], peer[r], m_slot)

    w_mate, w_near = {r: slot() for r in others}, slot()
    for r in others:
        landed(w_slot[r], full_share(r, share))
        push(full_share(r, share), full_share(r, share), mate, w_mate[r])
        push(full_share(r, share), full_share(r, share), sibling, w_near)

    def hand_weights(r):
        landed(w_mate[r], full_share(r, mate_share))
        push(full_share(r, mate_share), full_share(r, mate_share), sibling, w_near)

    o_far = slot()
    landed(o_first[1], out_part(1, 0))
    push(out_part(1, 0), out_part(1, 0), peer[2], o_far)
    landed(o_first[2], out_part(2, 1))
    push(out_part(2, 1), out_part(2, 1), peer[1], o_far)
    hand_weights(1)

    o_mate, o_near = {r: slot() for r in others}, {r: slot() for r in others}

    def spread_out(r):
        push(out_share(r, share), out_share(r, share), mate, o_mate[r])
        push(out_share(r, share), out_share(r, share), sibling, o_near[r])

    def hand_out(r):
        landed(o_mate[r], out_share(r, mate_share))
        push(out_share(r, mate_share), out_share(r, mate_share), sibling, o_near[r])

    landed(o_second[1], out_part(1, 1))
    spread_out(1)
    landed(o_second[2], out_part(2, 0))
    spread_out(2)
    hand_weights(2)
    x_far = slot()
    landed(x_first[1], x_part(1, 0))
    push(x_part(1, 0), x_part(3, 0), peer[2], x_far)
    landed(x_first[2], x_part(2, 1))
    push(x_part(2, 1), x_part(3, 1), peer[1], x_far)
    hand_weights(3)
    pltpu.make_async_copy(own_block, own_block, local_sem.at[6]).wait()
    landed(w_near, full.at[:, pl.ds(0, 6 * quarter), :])

    lane = lax.broadcasted_iota(jnp.int32, (1, 2 * HEAD), 1)
    scale = 1.0 / math.sqrt(HEAD)
    first = (lane < HEAD).astype(jnp.float32)
    keep = [(first * scale).astype(jnp.bfloat16), ((1.0 - first) * scale).astype(jnp.bfloat16)]

    def context_of(r):
        rows_in = x_all[r]
        queries, key_rows, value_rows = tuple(
            jnp.dot(rows_in, full[t], preferred_element_type=jnp.float32).astype(jnp.bfloat16)
            for t in range(3)
        )
        valid = meta[r, 1:2, :] > 0.0
        pieces = []
        for start in range(0, columns, 2 * HEAD):
            span = slice(start, start + 2 * HEAD)
            q_pair, k_pair, v_pair = queries[:, span], key_rows[:, span], value_rows[:, span]
            stacked = jnp.concatenate([q_pair * keep[0], q_pair * keep[1]], axis=0)
            scores = lax.dot_general(
                stacked, k_pair, (((1,), (1,)), ((), ())), preferred_element_type=jnp.float32
            )
            scores = jnp.where(valid, scores, -1000000000.0)
            expo = jnp.exp(scores - jnp.max(scores, axis=-1, keepdims=True))
            whole = jnp.sum(expo, axis=-1, keepdims=True)
            summed = jnp.dot(
                expo.astype(jnp.bfloat16), v_pair, preferred_element_type=jnp.float32
            )
            summed = summed / whole
            pieces.append(jnp.where(lane < HEAD, summed[:length], summed[length:]))
        return jnp.concatenate(pieces, axis=1).astype(jnp.bfloat16)

    def context_part(r, candidate, part):
        return context.at[r, candidate, pl.ds(part * half, half), :]

    def context_push(r, candidate, part, way, number):
        push(
            context_part(r, candidate, part),
            context_part(r ^ way, candidate ^ way, part),
            peer[way],
            number,
        )

    c_first = {(r, way): slot() for r in range(count) for way in (1, 2)}
    c_second = {r: slot() for r in range(count)}
    c_far = {r: slot() for r in range(count)}

    def product(r, candidate):
        return jnp.dot(
            context[r, candidate],
            out_full[row_block(peer[r][1]), :],
            preferred_element_type=jnp.float32,
        )

    def attend(r):
        context[0, r] = context_of(r)
        context_push(0, r, 0, 1, c_first[r, 1])
        context_push(0, r, 1, 2, c_first[r, 2])
        context_push(0, r, 1, 1, c_second[r])
        context_push(0, r, 0, 2, c_second[r])

    def begin(r):
        total[r] = product(0, r) + x_all[r].astype(jnp.float32)

    attend(0)
    begin(0)
    landed(m_slot, meta.at[pl.ds(1, count - 1)])
    landed(x_second[1], x_part(1, 1))
    attend(1)
    begin(1)
    landed(x_second[2], x_part(2, 0))
    attend(2)
    landed(o_far, out_share(3, share))
    spread_out(3)
    begin(2)
    hand_out(1)
    hand_out(2)
    landed(x_far, x_all.at[3])
    attend(3)
    begin(3)

    for r in range(count):
        landed(c_first[r, 1], context_part(1, r ^ 1, 0))
        context_push(1, r ^ 1, 0, 2, c_far[r ^ 3])
        landed(c_first[r, 2], context_part(2, r ^ 2, 1))
        context_push(2, r ^ 2, 1, 1, c_far[r ^ 3])
        if r == 0:
            for way in (1, 2):
                landed(o_near[way], out_full.at[pl.ds(0, 2 * quarter), :])
        landed(c_second[r], context.at[0, r])
        total[r ^ 1] += product(1, r ^ 1)
        total[r ^ 2] += product(2, r ^ 2)
        if r == 1:
            hand_out(3)
    landed(o_near[3], out_full.at[pl.ds(0, 2 * quarter), :])

    own_weight = meta[0, 0:1, :]
    own_column = jnp.broadcast_to(own_weight, (length, length)).T
    own_total = jnp.sum(own_weight, axis=1, keepdims=True)
    place = lax.broadcasted_iota(jnp.int32, utility_ref.shape, 1)

    def vectors_of(r):
        mixed = total[r] + product(3, r)
        centred = mixed - jnp.mean(mixed, axis=-1, keepdims=True)
        squares = jnp.sum(centred * centred, axis=-1, keepdims=True)
        return (centred / jnp.sqrt(squares + 0.001)).astype(jnp.bfloat16)

    def pair_of(own, far, r):
        far_weight = meta[r, 0:1, :]
        similar = lax.dot_general(
            own, far, (((1,), (1,)), ((), ())), preferred_element_type=jnp.float32
        )
        best_far = jnp.max(jnp.where(far_weight > 0, similar, -4.0), axis=1, keepdims=True)
        best_own = jnp.max(jnp.where(own_column > 0, similar, -4.0), axis=0, keepdims=True)
        forward = jnp.sum(own_column[:, 0:1] * best_far, axis=0, keepdims=True) / own_total
        backward = jnp.sum(far_weight * best_own, axis=1, keepdims=True) / jnp.sum(
            far_weight, axis=1, keepdims=True
        )
        return 0.5 * (forward + backward)

    vectors = {}
    for r in (3, 2, 1, 0):
        landed(c_far[r], context.at[3, r])
        vectors[r] = vectors_of(r)
    own = vectors[0]
    embedded_ref[...] = own
    utility = jnp.zeros(utility_ref.shape, jnp.float32)
    everything = jnp.zeros((1, 1), jnp.float32)
    for r in range(count):
        pair = pair_of(own, vectors[r], r)
        utility = jnp.where(place == peer[r][1], pair, utility)
        if r:
            everything = everything + pair
    utility_ref[...] = utility
    expected_ref[0] = everything[0, 0] / (count - 1)

    assert len(slots) <= SLOTS and sum(sent) == math.prod(drain.shape) * 2
    pltpu.make_async_copy(drain, drain, send_sem.at[0]).wait()


def shards(
    sizes,
    layer_input,
    token_ids,
    lengths,
    idf_table,
    query_weight,
    key_weight,
    value_weight,
    output_weight,
):
    local_cands, length, width = layer_input.shape
    count = sizes["cand"]
    rows = query_weight.shape[0]
    columns = width // count
    if (
        local_cands != 1
        or count != 4
        or sizes["src"] % 4
        or columns % (2 * HEAD)
        or rows % 64
        or length != 128
    ):
        return gathered_shards(
            layer_input,
            token_ids,
            lengths,
            idf_table,
            query_weight,
            key_weight,
            value_weight,
            output_weight,
        )
    anywhere = pl.BlockSpec(memory_space=pl.ANY)
    in_vmem = pl.BlockSpec(memory_space=pltpu.VMEM)
    in_smem = pl.BlockSpec(memory_space=pltpu.SMEM)
    sent = 12 * 3 * (rows // 4) * columns + 12 * (rows // 4) * width
    sent += 3 * length * width + 3 * 16 * length + 12 * length * columns
    embedded, utility, expected = pl.pallas_call(
        functools.partial(kernel, count),
        out_shape=(
            pltpu.VMEM((length, width), jnp.bfloat16),
            pltpu.VMEM((1, count), jnp.float32),
            pltpu.SMEM((1,), jnp.float32),
        ),
        in_specs=[anywhere] * 8,
        out_specs=(in_vmem, in_vmem, in_smem),
        scratch_shapes=[
            pltpu.VMEM((3, rows, width), jnp.bfloat16),
            pltpu.VMEM((3, rows * count, columns), jnp.bfloat16),
            pltpu.VMEM((rows * count, width), jnp.bfloat16),
            pltpu.VMEM((count, length, width), jnp.bfloat16),
            pltpu.VMEM((count, 8, length), jnp.float32),
            pltpu.VMEM((count, count, length, columns), jnp.bfloat16),
            pltpu.VMEM((count, length, width), jnp.float32),
            pltpu.VMEM((sent // 128, 128), jnp.bfloat16),
            pltpu.SMEM((1, length), jnp.int32),
            pltpu.SMEM((1,), jnp.int32),
            pltpu.SMEM(idf_table.shape, jnp.float32),
            pltpu.SemaphoreType.DMA((7,)),
            pltpu.SemaphoreType.DMA((1,)),
            pltpu.SemaphoreType.DMA((SLOTS,)),
            pltpu.SemaphoreType.REGULAR,
        ],
        compiler_params=pltpu.CompilerParams(collective_id=0, has_side_effects=True),
    )(
        layer_input.reshape(length, width),
        token_ids,
        lengths,
        idf_table,
        query_weight,
        key_weight,
        value_weight,
        output_weight,
    )
    return (embedded.reshape(1, length, width), utility, expected)


def solution(mesh):
    in_specs = (
        P(("src", "cand"), None, None),
        P(("src", "cand"), None),
        P(("src", "cand")),
        P("src"),
        P("cand", None),
        P("cand", None),
        P("cand", None),
        P("cand", None),
    )
    out_specs = (P(("src", "cand"), None, None), P(("src", "cand"), None), P(("src", "cand")))
    return jax.shard_map(
        functools.partial(shards, dict(mesh.shape)),
        mesh=mesh,
        in_specs=in_specs,
        out_specs=out_specs,
        check_vma=False,
    )
```

```python
import functools
import math

import jax
import jax.numpy as jnp
from jax import lax
from jax.experimental import pallas as pl
from jax.experimental.pallas import tpu as pltpu
from jax.sharding import PartitionSpec as P

HEAD = 64
SLOTS = 40


def block_utility(own_vectors, own_weight, far_vectors, far_weight):
    own_count, length, width = own_vectors.shape
    far_count = far_vectors.shape[0]
    similar = lax.dot_general(
        own_vectors.reshape(own_count * length, width),
        far_vectors.reshape(far_count * length, width),
        (((1,), (1,)), ((), ())),
        preferred_element_type=jnp.float32,
    )
    similar = similar.reshape(own_count, length, far_count, length)
    own_usable = own_weight > 0
    far_usable = far_weight > 0
    best_far = jnp.max(jnp.where(far_usable[None, None, :, :], similar, -4.0), axis=3)
    best_own = jnp.max(jnp.where(own_usable[:, :, None, None], similar, -4.0), axis=1)
    own_float = own_weight.astype(jnp.float32)
    far_float = far_weight.astype(jnp.float32)
    forward = jnp.einsum("il,ilj->ij", own_float, best_far, precision=lax.Precision.HIGHEST)
    forward = forward / jnp.sum(own_float, axis=1)[:, None]
    backward = jnp.einsum("jm,ijm->ij", far_float, best_own, precision=lax.Precision.HIGHEST)
    backward = backward / jnp.sum(far_float, axis=1)[None, :]
    return 0.5 * (forward + backward)


def gathered_shards(
    layer_input,
    token_ids,
    lengths,
    idf_table,
    query_weight,
    key_weight,
    value_weight,
    output_weight,
):
    local_cands, length, width = layer_input.shape
    cycle_size = lax.axis_size("cand")
    all_cands = local_cands * cycle_size
    head_size = HEAD
    head_count = width // head_size
    flat = layer_input.reshape(local_cands * length, width)
    pieces = (
        lax.all_gather(query_weight, "cand", axis=0, tiled=True),
        lax.all_gather(key_weight, "cand", axis=0, tiled=True),
        lax.all_gather(value_weight, "cand", axis=0, tiled=True),
    )
    columns = flat
    queries, key_rows, value_rows = tuple(
        (jnp.dot(columns, piece, preferred_element_type=jnp.float32) for piece in pieces)
    )
    queries = queries.astype(jnp.bfloat16).reshape(local_cands, length, head_count, head_size)
    key_rows = key_rows.astype(jnp.bfloat16).reshape(local_cands, length, head_count, head_size)
    value_rows = value_rows.astype(jnp.bfloat16).reshape(local_cands, length, head_count, head_size)
    positions = jnp.arange(length, dtype=jnp.int32)
    valid = positions[None, :] < lengths[:, None]
    scale = 1.0 / math.sqrt(head_size)
    scores = (
        jnp.einsum("clhe,cmhe->chlm", queries, key_rows, preferred_element_type=jnp.float32) * scale
    )
    scores = jnp.where(valid[:, None, None, :], scores, -1000000000.0)
    highest = jnp.max(scores, axis=-1, keepdims=True)
    expo = jnp.exp(scores - highest)
    probs = (expo / jnp.sum(expo, axis=-1, keepdims=True)).astype(jnp.bfloat16)
    context = jnp.einsum("chlm,cmhe->clhe", probs, value_rows, preferred_element_type=jnp.float32)
    context = context.astype(jnp.bfloat16).reshape(local_cands * length, width)
    columns = context
    mixed = jnp.dot(
        columns,
        lax.all_gather(output_weight, "cand", axis=0, tiled=True),
        preferred_element_type=jnp.float32,
    ) + flat.astype(jnp.float32)
    centred = mixed - jnp.mean(mixed, axis=-1, keepdims=True)
    squares = jnp.sum(centred * centred, axis=-1, keepdims=True)
    embedded = (
        (centred * (1.0 / jnp.sqrt(squares + 0.001)))
        .astype(jnp.bfloat16)
        .reshape(local_cands, length, width)
    )
    token_weight = (jnp.take(idf_table, token_ids, axis=0) * valid.astype(jnp.float32)).astype(
        jnp.bfloat16
    )
    myself = lax.axis_index("cand")
    piece = (
        lax.all_gather(embedded, "cand", axis=0, tiled=True),
        lax.all_gather(token_weight, "cand", axis=0, tiled=True),
    )
    utility = block_utility(embedded, token_weight, piece[0], piece[1])
    blocks = utility.reshape(local_cands, cycle_size, local_cands)
    own_part = lax.dynamic_slice(blocks, (0, myself, 0), (local_cands, 1, local_cands))[:, 0, :]
    diagonal = jnp.diagonal(own_part)
    expected_utility = (jnp.sum(utility, axis=1) - diagonal) / (all_cands - 1)
    return (embedded, utility, expected_utility)


def remote(src_ref, dst_ref, send_sem, recv_sem, device):
    return pltpu.make_async_remote_copy(
        src_ref=src_ref,
        dst_ref=dst_ref,
        send_sem=send_sem,
        recv_sem=recv_sem,
        device_id=device,
        device_id_type=pl.DeviceIdType.MESH,
    )


def flipped(index, bits):
    result = index
    place = 1
    while place <= bits:
        if bits & place:
            digit = lax.rem(lax.div(index, place), 2)
            result = result + place - 2 * place * digit
        place *= 2
    return result


def kernel(
    count,
    x_hbm,
    ids_hbm,
    used_hbm,
    table_hbm,
    q_hbm,
    k_hbm,
    v_hbm,
    o_hbm,
    embedded_ref,
    utility_ref,
    expected_ref,
    stage,
    full,
    out_full,
    x_all,
    meta,
    context,
    total,
    drain,
    ids,
    used,
    table,
    local_sem,
    send_sem,
    recv_sem,
    ready_sem,
):
    group, me = lax.axis_index("src"), lax.axis_index("cand")
    share = lax.rem(group, 4)
    sibling = (flipped(group, 1), me)
    mate = (flipped(group, 2), me)
    others = range(1, count)
    peer = [(group, flipped(me, bits)) for bits in range(count)]
    length, width = x_hbm.shape
    rows, columns = stage.shape[1], full.shape[2]
    quarter, half = rows // 4, length // 2
    sent, slots = [], []

    def signal(semaphore, device):
        pl.semaphore_signal(
            semaphore, inc=1, device_id=device, device_id_type=pl.DeviceIdType.MESH
        )

    def slot():
        slots.append(len(slots))
        return slots[-1]

    def push(src_ref, dst_ref, device, number):
        remote(src_ref, dst_ref, send_sem.at[0], recv_sem.at[number], device).start()
        sent.append(math.prod(src_ref.shape) * src_ref.dtype.itemsize)

    def landed(number, like):
        pltpu.make_async_copy(like, like, recv_sem.at[number]).wait()

    def column_block(index):
        return pl.ds(pl.multiple_of(index * columns, columns), columns)

    def row_block(index):
        return pl.ds(pl.multiple_of(index * rows, rows), rows)

    def row_share(index, which):
        return pl.ds(pl.multiple_of(index * rows + which * quarter, quarter), quarter)

    own_share = pl.ds(pl.multiple_of(share * quarter, quarter), quarter)
    mate_share = lax.rem(share + 2, 4)

    weights = (q_hbm, k_hbm, v_hbm)
    own_rows = out_full.at[row_block(me), :]
    own_block = full.at[:, row_block(me), :]
    for t, w in enumerate(weights):
        pltpu.make_async_copy(w, stage.at[t], local_sem.at[0]).start()
    load_o = pltpu.make_async_copy(o_hbm, own_rows, local_sem.at[1])
    load_x = pltpu.make_async_copy(x_hbm, x_all.at[0], local_sem.at[2])
    small = [
        pltpu.make_async_copy(used_hbm, used, local_sem.at[3]),
        pltpu.make_async_copy(ids_hbm, ids, local_sem.at[4]),
        pltpu.make_async_copy(table_hbm, table, local_sem.at[5]),
    ]
    load_o.start()
    load_x.start()
    for load in small:
        load.start()
    for t, w in enumerate(weights):
        pltpu.make_async_copy(
            w.at[:, column_block(me)], full.at[t, row_block(me), :], local_sem.at[6]
        ).start()

    barrier = pltpu.get_barrier_semaphore()
    targets = [sibling, mate, peer[1], peer[2]]
    for target in targets:
        signal(barrier, target)
    pl.semaphore_wait(barrier, len(targets))
    signal(ready_sem, peer[1])

    def full_share(r, which):
        return full.at[:, row_share(peer[r][1], which), :]

    def out_share(r, which):
        return out_full.at[row_share(peer[r][1], which), :]

    def out_part(r, part):
        start = peer[r][1] * rows + share * quarter + part * (quarter // 2)
        return out_full.at[pl.ds(pl.multiple_of(start, quarter // 2), quarter // 2), :]

    def x_part(r, part):
        return x_all.at[r, pl.ds(part * half, half), :]

    w_slot = {r: slot() for r in others}

    def send_weights(r):
        push(
            stage.at[:, own_share, column_block(peer[r][1])],
            full_share(0, share),
            peer[r],
            w_slot[r],
        )

    pltpu.make_async_copy(stage, stage, local_sem.at[0]).wait()
    send_weights(1)
    send_weights(2)
    pl.semaphore_wait(ready_sem, 1)
    send_weights(3)
    load_o.wait()
    o_first, o_second = {1: slot(), 2: slot()}, {1: slot(), 2: slot()}
    push(out_part(0, 0), out_part(0, 0), peer[1], o_first[1])
    push(out_part(0, 1), out_part(0, 1), peer[2], o_first[2])
    push(out_part(0, 1), out_part(0, 1), peer[1], o_second[1])
    push(out_part(0, 0), out_part(0, 0), peer[2], o_second[2])
    load_x.wait()
    x_first, x_second = {1: slot(), 2: slot()}, {1: slot(), 2: slot()}
    push(x_part(0, 0), x_part(1, 0), peer[1], x_first[1])
    push(x_part(0, 1), x_part(2, 1), peer[2], x_first[2])
    push(x_part(0, 1), x_part(1, 1), peer[1], x_second[1])
    push(x_part(0, 0), x_part(2, 0), peer[2], x_second[2])

    position = lax.broadcasted_iota(jnp.int32, (1, length), 1)

    def look_up(at, weights_row):
        return jnp.where(position == at, table[ids[0, at]], weights_row)

    for load in small:
        load.wait()
    valid_row = (position < used[0]).astype(jnp.float32)
    weights_row = lax.fori_loop(0, length, look_up, jnp.zeros((1, length), jnp.float32), unroll=8)
    weights_row = (weights_row * valid_row).astype(jnp.bfloat16).astype(jnp.float32)
    meta[0] = jnp.concatenate([weights_row, jnp.broadcast_to(valid_row, (7, length))], axis=0)
    m_slot = slot()
    for r in others:
        push(meta.at[0], meta.at[r], peer[r], m_slot)

    w_mate, w_near = {r: slot() for r in others}, slot()
    for r in others:
        landed(w_slot[r], full_share(r, share))
        push(full_share(r, share), full_share(r, share), mate, w_mate[r])
        push(full_share(r, share), full_share(r, share), sibling, w_near)

    def hand_weights(r):
        landed(w_mate[r], full_share(r, mate_share))
        push(full_share(r, mate_share), full_share(r, mate_share), sibling, w_near)

    o_far = slot()
    landed(o_first[1], out_part(1, 0))
    push(out_part(1, 0), out_part(1, 0), peer[2], o_far)
    landed(o_first[2], out_part(2, 1))
    push(out_part(2, 1), out_part(2, 1), peer[1], o_far)
    hand_weights(1)

    o_mate, o_near = {r: slot() for r in others}, {r: slot() for r in others}

    def spread_out(r):
        push(out_share(r, share), out_share(r, share), mate, o_mate[r])
        push(out_share(r, share), out_share(r, share), sibling, o_near[r])

    def hand_out(r):
        landed(o_mate[r], out_share(r, mate_share))
        push(out_share(r, mate_share), out_share(r, mate_share), sibling, o_near[r])

    landed(o_second[1], out_part(1, 1))
    spread_out(1)
    landed(o_second[2], out_part(2, 0))
    spread_out(2)
    hand_weights(2)
    x_far = slot()
    landed(x_first[1], x_part(1, 0))
    push(x_part(1, 0), x_part(3, 0), peer[2], x_far)
    landed(x_first[2], x_part(2, 1))
    push(x_part(2, 1), x_part(3, 1), peer[1], x_far)
    hand_weights(3)
    pltpu.make_async_copy(own_block, own_block, local_sem.at[6]).wait()
    landed(w_near, full.at[:, pl.ds(0, 6 * quarter), :])

    lane = lax.broadcasted_iota(jnp.int32, (1, 2 * HEAD), 1)
    scale = 1.0 / math.sqrt(HEAD)
    first = (lane < HEAD).astype(jnp.float32)
    keep = [(first * scale).astype(jnp.bfloat16), ((1.0 - first) * scale).astype(jnp.bfloat16)]

    def context_of(r):
        rows_in = x_all[r]
        queries, key_rows, value_rows = tuple(
            jnp.dot(rows_in, full[t], preferred_element_type=jnp.float32).astype(jnp.bfloat16)
            for t in range(3)
        )
        valid = meta[r, 1:2, :] > 0.0
        pieces = []
        for start in range(0, columns, 2 * HEAD):
            span = slice(start, start + 2 * HEAD)
            q_pair, k_pair, v_pair = queries[:, span], key_rows[:, span], value_rows[:, span]
            stacked = jnp.concatenate([q_pair * keep[0], q_pair * keep[1]], axis=0)
            scores = lax.dot_general(
                stacked, k_pair, (((1,), (1,)), ((), ())), preferred_element_type=jnp.float32
            )
            scores = jnp.where(valid, scores, -1000000000.0)
            expo = jnp.exp(scores - jnp.max(scores, axis=-1, keepdims=True))
            whole = jnp.sum(expo, axis=-1, keepdims=True)
            summed = jnp.dot(
                expo.astype(jnp.bfloat16), v_pair, preferred_element_type=jnp.float32
            )
            summed = summed / whole
            pieces.append(jnp.where(lane < HEAD, summed[:length], summed[length:]))
        return jnp.concatenate(pieces, axis=1).astype(jnp.bfloat16)

    def context_part(r, candidate, part):
        return context.at[r, candidate, pl.ds(part * half, half), :]

    def context_push(r, candidate, part, way, number):
        push(
            context_part(r, candidate, part),
            context_part(r ^ way, candidate ^ way, part),
            peer[way],
            number,
        )

    c_first = {(r, way): slot() for r in range(count) for way in (1, 2)}
    c_second = {r: slot() for r in range(count)}
    c_far = {r: slot() for r in range(count)}

    def product(r, candidate):
        return jnp.dot(
            context[r, candidate],
            out_full[row_block(peer[r][1]), :],
            preferred_element_type=jnp.float32,
        )

    def attend(r):
        context[0, r] = context_of(r)
        context_push(0, r, 0, 1, c_first[r, 1])
        context_push(0, r, 1, 2, c_first[r, 2])
        context_push(0, r, 1, 1, c_second[r])
        context_push(0, r, 0, 2, c_second[r])

    def begin(r):
        total[r] = product(0, r) + x_all[r].astype(jnp.float32)

    attend(0)
    begin(0)
    landed(m_slot, meta.at[pl.ds(1, count - 1)])
    landed(x_second[1], x_part(1, 1))
    attend(1)
    begin(1)
    landed(x_second[2], x_part(2, 0))
    attend(2)
    landed(o_far, out_share(3, share))
    spread_out(3)
    begin(2)
    hand_out(1)
    hand_out(2)
    landed(x_far, x_all.at[3])
    attend(3)
    begin(3)

    for r in range(count):
        landed(c_first[r, 1], context_part(1, r ^ 1, 0))
        context_push(1, r ^ 1, 0, 2, c_far[r ^ 3])
        landed(c_first[r, 2], context_part(2, r ^ 2, 1))
        context_push(2, r ^ 2, 1, 1, c_far[r ^ 3])
        if r == 0:
            for way in (1, 2):
                landed(o_near[way], out_full.at[pl.ds(0, 2 * quarter), :])
        landed(c_second[r], context.at[0, r])
        total[r ^ 1] += product(1, r ^ 1)
        total[r ^ 2] += product(2, r ^ 2)
        if r == 1:
            hand_out(3)
    landed(o_near[3], out_full.at[pl.ds(0, 2 * quarter), :])

    weight_of = [meta[r, 0:1, :] for r in range(count)]
    sum_of = [jnp.sum(weights_row, axis=1, keepdims=True) for weights_row in weight_of]
    own_column = jnp.broadcast_to(weight_of[0], (length, length)).T
    own_usable = own_column > 0
    column = own_column[:, 0:1]
    place = lax.broadcasted_iota(jnp.int32, utility_ref.shape, 1)

    def vectors_of(r):
        mixed = total[r] + product(3, r)
        centred = mixed - jnp.mean(mixed, axis=-1, keepdims=True)
        squares = jnp.sum(centred * centred, axis=-1, keepdims=True)
        return (centred * (1.0 / jnp.sqrt(squares + 0.001))).astype(jnp.bfloat16)

    def pair_of(own, far, r):
        similar = lax.dot_general(
            own, far, (((1,), (1,)), ((), ())), preferred_element_type=jnp.float32
        )
        best_far = jnp.max(jnp.where(weight_of[r] > 0, similar, -4.0), axis=1, keepdims=True)
        best_own = jnp.max(jnp.where(own_usable, similar, -4.0), axis=0, keepdims=True)
        forward = jnp.sum(column * best_far, axis=0, keepdims=True) / sum_of[0]
        backward = jnp.sum(weight_of[r] * best_own, axis=1, keepdims=True) / sum_of[r]
        return 0.5 * (forward + backward)

    vectors = {}
    for r in (3, 2, 1, 0):
        landed(c_far[r], context.at[3, r])
        vectors[r] = vectors_of(r)
        if r == 0:
            embedded_ref[...] = vectors[0]
    pair = [pair_of(vectors[0], vectors[r], r) for r in range(count)]
    utility = jnp.zeros(utility_ref.shape, jnp.float32)
    for r in range(count):
        utility = jnp.where(place == peer[r][1], pair[r], utility)
    utility_ref[...] = utility
    expected_ref[0] = (pair[1] + pair[2] + pair[3])[0, 0] / (count - 1)

    assert len(slots) <= SLOTS and sum(sent) == math.prod(drain.shape) * 2
    pltpu.make_async_copy(drain, drain, send_sem.at[0]).wait()


def shards(
    sizes,
    layer_input,
    token_ids,
    lengths,
    idf_table,
    query_weight,
    key_weight,
    value_weight,
    output_weight,
):
    local_cands, length, width = layer_input.shape
    count = sizes["cand"]
    rows = query_weight.shape[0]
    columns = width // count
    if (
        local_cands != 1
        or count != 4
        or sizes["src"] % 4
        or columns % (2 * HEAD)
        or rows % 64
        or length != 128
    ):
        return gathered_shards(
            layer_input,
            token_ids,
            lengths,
            idf_table,
            query_weight,
            key_weight,
            value_weight,
            output_weight,
        )
    anywhere = pl.BlockSpec(memory_space=pl.ANY)
    in_vmem = pl.BlockSpec(memory_space=pltpu.VMEM)
    in_smem = pl.BlockSpec(memory_space=pltpu.SMEM)
    sent = 12 * 3 * (rows // 4) * columns + 12 * (rows // 4) * width
    sent += 3 * length * width + 3 * 16 * length + 12 * length * columns
    embedded, utility, expected = pl.pallas_call(
        functools.partial(kernel, count),
        out_shape=(
            pltpu.VMEM((length, width), jnp.bfloat16),
            pltpu.VMEM((1, count), jnp.float32),
            pltpu.SMEM((1,), jnp.float32),
        ),
        in_specs=[anywhere] * 8,
        out_specs=(in_vmem, in_vmem, in_smem),
        scratch_shapes=[
            pltpu.VMEM((3, rows, width), jnp.bfloat16),
            pltpu.VMEM((3, rows * count, columns), jnp.bfloat16),
            pltpu.VMEM((rows * count, width), jnp.bfloat16),
            pltpu.VMEM((count, length, width), jnp.bfloat16),
            pltpu.VMEM((count, 8, length), jnp.float32),
            pltpu.VMEM((count, count, length, columns), jnp.bfloat16),
            pltpu.VMEM((count, length, width), jnp.float32),
            pltpu.VMEM((sent // 128, 128), jnp.bfloat16),
            pltpu.SMEM((1, length), jnp.int32),
            pltpu.SMEM((1,), jnp.int32),
            pltpu.SMEM(idf_table.shape, jnp.float32),
            pltpu.SemaphoreType.DMA((7,)),
            pltpu.SemaphoreType.DMA((1,)),
            pltpu.SemaphoreType.DMA((SLOTS,)),
            pltpu.SemaphoreType.REGULAR,
        ],
        compiler_params=pltpu.CompilerParams(collective_id=0, has_side_effects=True),
    )(
        layer_input.reshape(length, width),
        token_ids,
        lengths,
        idf_table,
        query_weight,
        key_weight,
        value_weight,
        output_weight,
    )
    return (embedded.reshape(1, length, width), utility, expected)


def solution(mesh):
    in_specs = (
        P(("src", "cand"), None, None),
        P(("src", "cand"), None),
        P(("src", "cand")),
        P("src"),
        P("cand", None),
        P("cand", None),
        P("cand", None),
        P("cand", None),
    )
    out_specs = (P(("src", "cand"), None, None), P(("src", "cand"), None), P(("src", "cand")))
    return jax.shard_map(
        functools.partial(shards, dict(mesh.shape)),
        mesh=mesh,
        in_specs=in_specs,
        out_specs=out_specs,
        check_vma=False,
    )
```
